32 devices in a mesh: grp: 2 (over x), tile: 16 (over z, y, core).
Axes of the slice: x: 2, y: 2, z: 4, core: 2. Of those that a mesh axis runs over, the one named last changes fastest.
Arguments:
- visibility: bfloat16 [2, 512, 512, 1024], P(None, 'tile', None, 'grp'), may hold values from -3 to 3, as said below
- dish_pair_okay: int32 [512, 512], P('tile'), may hold values 0 or 1
- triangles: int32 [3, 32768], P(None, 'tile'), may hold values from 0 to 511, as said below
Outputs:
- triangle_means: float32 [2, 32768], P(None, 'tile')
- closure_spectrum: float32 [2, 1024], P(None, ('grp', 'tile'))
The draws below stay inside these ranges and needn't reach their ends.
Inputs may be any that keep to these rules, and one draw needn't show every extreme that they name: Both parts of every visibility lie in -3 to 3. `triangles`: column j belongs to block d = j // 2048 and level k = (j % 2048) // 1024; its first antenna lies in block d (antennas d * 32 to d * 32 + 31), its second in block d XOR 2**k, and its third is any antenna other than the first two.
All inputs are finite; a program needn't handle non-finite values. No bound on the sum of `dish_pair_okay` on one device may be relied on, other than what follows from the above.
Results may differ from the reference program's by a relative error of at most 0.0003.
Values may be sent and summed in bfloat16 or wider, within the bound.
A program may use at most 128 MiB of HBM per device.

```python
import math
import jax
import jax.numpy as jnp
from jax import lax

RECEIVER_DISHES = 512
RADIO_BANDS = 1024
TRI_LVL = 1024
TA = 32
TRI_DEV = 2048
THREE_DISH_SETS = 32768


def draw_visibility(key, part):
    seed_sequence = jax.random.split(key, 3)
    rotation_angles = jax.random.uniform(seed_sequence[0], (RECEIVER_DISHES, RADIO_BANDS), jnp.float32, -math.pi, math.pi)
    loudness_scale = 0.8 + 0.4 * jax.random.uniform(seed_sequence[1], (RECEIVER_DISHES, RADIO_BANDS), jnp.float32)
    hiss_component = 0.3 * jnp.clip(jax.random.normal(seed_sequence[2], (2, RECEIVER_DISHES, RECEIVER_DISHES, RADIO_BANDS), jnp.float32), -4.0, 4.0)
    gain_real = loudness_scale * jnp.cos(rotation_angles)
    gain_imag = loudness_scale * jnp.sin(rotation_angles)
    signal_real = gain_real[:, None, :] * gain_real[None, :, :] + gain_imag[:, None, :] * gain_imag[None, :, :]
    signal_imag = gain_imag[:, None, :] * gain_real[None, :, :] - gain_real[:, None, :] * gain_imag[None, :, :]
    return (jnp.stack([signal_real, signal_imag]) + hiss_component).astype(jnp.bfloat16)


def draw_triangles(key, part):
    seed_sequence = jax.random.split(key, 3)
    column = jnp.arange(THREE_DISH_SETS, dtype=jnp.int32)
    block_index = column // TRI_DEV
    level_index = column % TRI_DEV // TRI_LVL
    partner = jnp.bitwise_xor(block_index, jnp.left_shift(jnp.ones_like(level_index), level_index))
    first = block_index * TA + jax.random.randint(seed_sequence[0], (THREE_DISH_SETS,), 0, TA, jnp.int32)
    second = partner * TA + jax.random.randint(seed_sequence[1], (THREE_DISH_SETS,), 0, TA, jnp.int32)
    lower = jnp.minimum(first, second)
    upper = jnp.maximum(first, second)
    vertex_point = jax.random.randint(seed_sequence[2], (THREE_DISH_SETS,), 0, RECEIVER_DISHES - 2, jnp.int32)
    vertex_point = vertex_point + (vertex_point >= lower).astype(jnp.int32)
    vertex_point = vertex_point + (vertex_point >= upper).astype(jnp.int32)
    return jnp.stack([first, second, vertex_point]).astype(jnp.int32)


def place_ends(result, own_key, low, largest):
    spot = [jax.random.randint(jax.random.fold_in(own_key, axis), (), 0, length) for axis, length in enumerate(result.shape)]
    widest = result.shape.index(max(result.shape))
    beside = spot[:widest] + [(spot[widest] + 1) % result.shape[widest]] + spot[widest + 1:]
    return result.at[tuple(spot)].set(low).at[tuple(beside)].set(largest)


def setup_inputs(seed: int = 0) -> dict:
    seeds = jax.random.split(jax.random.key(seed), 4)
    return {
        "visibility": draw_visibility(jax.random.fold_in(seeds[3], 71), 0),
        "dish_pair_okay": place_ends((jax.random.randint(seeds[1], (RECEIVER_DISHES, RECEIVER_DISHES), 0, 8) < 7).astype(jnp.int32), jax.random.fold_in(seeds[1], 1), 0, 1),
        "triangles": draw_triangles(jax.random.fold_in(seeds[3], 71), 0),
    }


def bispectrum(edge_ab, edge_bc, edge_ac):
    edge_ab = edge_ab.astype(jnp.float32)
    edge_bc = edge_bc.astype(jnp.float32)
    edge_ac = edge_ac.astype(jnp.float32)
    prod_real = edge_ab[0] * edge_bc[0] - edge_ab[1] * edge_bc[1]
    prod_imag = edge_ab[0] * edge_bc[1] + edge_ab[1] * edge_bc[0]
    real_part = prod_real * edge_ac[0] + prod_imag * edge_ac[1]
    imag_part = prod_imag * edge_ac[0] - prod_real * edge_ac[1]
    return (real_part, imag_part)

def reference(visibility, dish_pair_okay, triangles):
    flag_table = dish_pair_okay.astype(jnp.float32)
    count = triangles.shape[1] // TRI_LVL
    blocks = jnp.transpose(triangles.reshape(3, count, TRI_LVL), (1, 0, 2))

    def step(carry, block):
        first, second, vertex_point = (block[0], block[1], block[2])
        edge_ab = visibility[:, first, second, :]
        edge_bc = visibility[:, second, vertex_point, :]
        edge_ac = visibility[:, first, vertex_point, :]
        weight = flag_table[first, second] * flag_table[second, vertex_point] * flag_table[first, vertex_point]
        real_part, imag_part = bispectrum(edge_ab, edge_bc, edge_ac)
        weighted_real = weight[:, None] * real_part
        weighted_imag = weight[:, None] * imag_part
        magnitude = weight[:, None] * jnp.sqrt(real_part * real_part + imag_part * imag_part)
        new_carry = (carry[0] + lax.optimization_barrier(jnp.sum(weighted_real, 0)), carry[1] + lax.optimization_barrier(jnp.sum(weighted_imag, 0)), carry[2] + lax.optimization_barrier(jnp.sum(magnitude, 0)))
        means = jnp.stack([lax.optimization_barrier(jnp.sum(weighted_real, 1)), lax.optimization_barrier(jnp.sum(weighted_imag, 1))]) / RADIO_BANDS
        return (new_carry, means)
    start = (jnp.zeros((RADIO_BANDS,), jnp.float32), jnp.zeros((RADIO_BANDS,), jnp.float32), jnp.zeros((RADIO_BANDS,), jnp.float32))
    totals, means = lax.scan(step, start, blocks)
    triangle_means = jnp.transpose(means, (1, 0, 2)).reshape(2, count * TRI_LVL)
    closure_spectrum = jnp.stack([totals[0], totals[1]]) / (1.0 + totals[2])
    return (triangle_means, closure_spectrum)
```

```python
import functools

import jax
import jax.numpy as jnp
from jax import lax
from jax.experimental import pallas as pl
from jax.experimental.pallas import tpu as pltpu
from jax.sharding import PartitionSpec as P

TRI_LVL = 1024
LANES = 128
GATHER = 256
BLOCK = 128


def swapped(array, axis, stride):
    return lax.ppermute(array, axis, [(i, i ^ 1 << stride) for i in range(lax.axis_size(axis))])


def gather_kernel(index, flags, vis, *refs, dishes, phases):
    outs, (table, turn) = refs[: len(phases)], refs[len(phases) :]
    step = pl.program_id(0)
    cols, channels = vis.shape[2], vis.shape[3]
    chunks = channels // LANES
    kinds = 2 * chunks
    blank = dishes * cols
    group = 16
    unroll = turn.shape[0]

    @pl.when(step == 0)
    def _():
        table[blank] = jnp.zeros((kinds, LANES), table.dtype)

    @pl.when(step < dishes)
    def _():
        def turn_rows(it, _):
            for u in range(unroll):
                start = pl.multiple_of((it * unroll + u) * group, group)
                for c in range(chunks):
                    for plane in range(2):
                        x = vis[plane, 0, pl.ds(start, group), pl.ds(c * LANES, LANES)]
                        turn[u, pl.ds(2 * c + plane, group, stride=kinds), :] = x.astype(jnp.float32)
            for u in range(unroll):
                start = (it * unroll + u) * group
                y = turn[u].reshape(group, kinds, LANES)
                table[pl.ds(step * cols + start, group)] = y.astype(table.dtype)
            return 0

        lax.fori_loop(0, cols // (group * unroll), turn_rows, 0)

    first = 0
    for out, count in zip(outs, phases):
        low = dishes + first // GATHER

        @pl.when((step >= low) & (step < low + count // GATHER))
        def _(out=out):
            base = (step - dishes) * GATHER

            def copy_rows(it, _):
                for u in range(16):
                    j = it * 16 + u
                    row = index[base + j]
                    row = jnp.where(flags[row] != 0, row, blank)
                    out[j] = table[row]
                return 0

            lax.fori_loop(0, GATHER // 16, copy_rows, 0)

        first += count


def gather_rows(visibility, flags, index, phases):
    _, dishes, cols, channels = visibility.shape
    kinds = 2 * channels // LANES
    steps = dishes + sum(phases) // GATHER
    out_specs, first = [], dishes
    for count in phases:
        n = count // GATHER
        out_specs.append(
            pl.BlockSpec((GATHER, kinds, LANES), lambda i, lo=first, n=n: (jnp.clip(i - lo, 0, n - 1), 0, 0))
        )
        first += n
    return pl.pallas_call(
        functools.partial(gather_kernel, dishes=dishes, phases=phases),
        grid=(steps,),
        in_specs=[
            pl.BlockSpec(memory_space=pltpu.SMEM),
            pl.BlockSpec(memory_space=pltpu.SMEM),
            pl.BlockSpec((2, 1, cols, channels), lambda i: (0, jnp.minimum(i, dishes - 1), 0, 0)),
        ],
        out_specs=out_specs,
        out_shape=[jax.ShapeDtypeStruct((count, kinds, LANES), visibility.dtype) for count in phases],
        scratch_shapes=[
            pltpu.VMEM((dishes * cols + 1, kinds, LANES), visibility.dtype),
            pltpu.VMEM((4, 16 * kinds, LANES), jnp.float32),
        ],
        compiler_params=pltpu.CompilerParams(
            dimension_semantics=("arbitrary",), vmem_limit_bytes=52 * 1024 * 1024
        ),
        name="gather_rows",
    )(index, flags, visibility)


def triangle_kernel(ab, ac, bc, sums, spec, wide, line):
    kinds = ab.shape[1]
    chunks = kinds // 2
    group = 16

    @pl.when(pl.program_id(0) == 0)
    def _():
        spec[...] = jnp.zeros(spec.shape, spec.dtype)

    def fold(x):
        return x[:8] + x[8:]

    def some(it, acc):
        acc = list(acc)
        for u in range(2):
            start = pl.multiple_of((it * 2 + u) * group, group)
            for e, ref in enumerate((ab, bc, ac)):
                rows = ref[pl.ds(start, group)].astype(jnp.float32)
                wide[u, e] = rows.reshape(group * kinds, LANES)
            total_real = total_imag = None
            for c in range(chunks):
                (a_r, a_i), (b_r, b_i), (c_r, c_i) = [
                    [wide[u, e, pl.ds(2 * c + plane, group, stride=kinds), :] for plane in range(2)]
                    for e in range(3)
                ]
                p_r = a_r * b_r - a_i * b_i
                p_i = a_r * b_i + a_i * b_r
                real = p_r * c_r + p_i * c_i
                imag = p_i * c_r - p_r * c_i
                norm = jnp.sqrt(real * real + imag * imag)
                acc[3 * c] = acc[3 * c] + fold(real)
                acc[3 * c + 1] = acc[3 * c + 1] + fold(imag)
                acc[3 * c + 2] = acc[3 * c + 2] + fold(norm)
                total_real = real if c == 0 else total_real + real
                total_imag = imag if c == 0 else total_imag + imag
            line[0, pl.ds(start, group), :] = total_real
            line[1, pl.ds(start, group), :] = total_imag
        return tuple(acc)

    zero = jnp.zeros((8, LANES), jnp.float32)
    acc = lax.fori_loop(0, BLOCK // (2 * group), some, (zero,) * (3 * chunks))
    for c in range(chunks):
        for part in range(3):
            spec[part, c] = spec[part, c] + acc[3 * c + part]
    ones = jnp.ones((8, LANES), jnp.float32)
    for part in range(2):
        lane_sum = lax.dot_general(
            ones,
            line[part],
            (((1,), (1,)), ((), ())),
            precision=lax.Precision.HIGHEST,
            preferred_element_type=jnp.float32,
        )
        sums[pl.ds(part, 1), :] = lane_sum[:1]


def triangle_sums(own, bc, level):
    count, kinds, _ = bc.shape
    n = count // BLOCK
    block = (BLOCK, kinds, LANES)
    return pl.pallas_call(
        triangle_kernel,
        grid=(n,),
        in_specs=[
            pl.BlockSpec(block, lambda i: (2 * level * n + i, 0, 0)),
            pl.BlockSpec(block, lambda i: ((2 * level + 1) * n + i, 0, 0)),
            pl.BlockSpec(block, lambda i: (i, 0, 0)),
        ],
        out_specs=[
            pl.BlockSpec((2, BLOCK), lambda i: (0, i)),
            pl.BlockSpec((3, kinds // 2, 8, LANES), lambda i: (0, 0, 0, 0)),
        ],
        out_shape=[
            jax.ShapeDtypeStruct((2, count), jnp.float32),
            jax.ShapeDtypeStruct((3, kinds // 2, 8, LANES), jnp.float32),
        ],
        scratch_shapes=[
            pltpu.VMEM((2, 3, 16 * kinds, LANES), jnp.float32),
            pltpu.VMEM((2, BLOCK, LANES), jnp.float32),
        ],
        compiler_params=pltpu.CompilerParams(dimension_semantics=("arbitrary",)),
        name="triangle_sums",
    )(own, own, bc)


def body(visibility, dish_pair_okay, triangles):
    _, block_rows, cols, channels = visibility.shape
    levels = triangles.shape[1] // TRI_LVL
    tiles = lax.axis_size("tile")
    device = lax.axis_index("tile")
    asked, own = [], []
    for level in range(levels):
        block = triangles[:, level * TRI_LVL : (level + 1) * TRI_LVL]
        partner = jnp.bitwise_xor(device, 1 << level)
        first_local = block[0] - device * block_rows
        second_local = block[1] - partner * block_rows
        asked.append(swapped(second_local * cols + block[2], "tile", level))
        own += [first_local * cols + block[1], first_local * cols + block[2]]
    order = list(reversed(range(levels)))
    index = jnp.concatenate([asked[level] for level in order] + own)
    phases = (TRI_LVL,) * levels + (2 * levels * TRI_LVL,)
    *picked, own_rows = gather_rows(visibility, dish_pair_okay.reshape(-1), index, phases)
    arrived = {level: swapped(rows, "tile", level) for level, rows in zip(order, picked)}
    parts = [triangle_sums(own_rows, arrived[level], level) for level in range(levels)]
    joined = lax.psum(jnp.concatenate([sums for sums, _ in parts], axis=1), "grp")
    triangle_means = joined / (channels * lax.axis_size("grp"))
    spec = sum(part for _, part in parts).sum(2).reshape(3, tiles, channels // tiles)
    spec = lax.all_to_all(spec.transpose(1, 0, 2), "tile", 0, 0).sum(0)
    closure_spectrum = spec[:2] / (1.0 + spec[2:])
    return (triangle_means, closure_spectrum)


def solution(mesh):
    placed = (P(None, "tile", None, "grp"), P("tile", None), P(None, "tile"))
    return jax.shard_map(
        body,
        mesh=mesh,
        in_specs=placed,
        out_specs=(P(None, "tile"), P(None, ("grp", "tile"))),
        check_vma=False,
    )
```

```python
import functools

import jax
import jax.numpy as jnp
from jax import lax
from jax.experimental import pallas as pl
from jax.experimental.pallas import tpu as pltpu
from jax.sharding import PartitionSpec as P


TRI_LVL = 1024
LANES = 128
GATHER = 256
BLOCK = 128


def swapped(array, axis, stride):
    return lax.ppermute(array, axis, [(i, i ^ 1 << stride) for i in range(lax.axis_size(axis))])


def turn_kernel(vis, table, turn):
    step = pl.program_id(0)
    cols, channels = vis.shape[2], vis.shape[3]
    chunks = channels // LANES
    kinds = 2 * chunks
    group = 16
    unroll = turn.shape[0]

    @pl.when(step == 0)
    def _():
        table[table.shape[0] - 1] = jnp.zeros((kinds, LANES), table.dtype)

    def turn_rows(it, _):
        for u in range(unroll):
            start = pl.multiple_of((it * unroll + u) * group, group)
            for c in range(chunks):
                for plane in range(2):
                    x = vis[plane, 0, pl.ds(start, group), pl.ds(c * LANES, LANES)]
                    turn[u, pl.ds(2 * c + plane, group, stride=kinds), :] = x.astype(jnp.float32)
        for u in range(unroll):
            start = (it * unroll + u) * group
            y = turn[u].reshape(group, kinds, LANES)
            table[pl.ds(step * cols + start, group)] = y.astype(table.dtype)
        return 0

    lax.fori_loop(0, cols // (group * unroll), turn_rows, 0)


def turned(visibility):
    _, dishes, cols, channels = visibility.shape
    kinds = 2 * channels // LANES
    return pl.pallas_call(
        turn_kernel,
        grid=(dishes,),
        in_specs=[pl.BlockSpec((2, 1, cols, channels), lambda i: (0, i, 0, 0))],
        out_specs=pl.BlockSpec(memory_space=pltpu.VMEM),
        out_shape=pltpu.VMEM((dishes * cols + 1, kinds, LANES), visibility.dtype),
        scratch_shapes=[pltpu.VMEM((4, 16 * kinds, LANES), jnp.float32)],
        compiler_params=pltpu.CompilerParams(
            dimension_semantics=("arbitrary",), vmem_limit_bytes=8 * 1024 * 1024
        ),
        name="turned",
    )(visibility)


def gather_kernel(index, flags, table, *outs, phases):
    step = pl.program_id(0)
    blank = table.shape[0] - 1
    first = 0
    for out, count in zip(outs, phases):
        low = first // GATHER

        @pl.when((step >= low) & (step < low + count // GATHER))
        def _(out=out):
            base = step * GATHER

            def copy_rows(it, _):
                for u in range(16):
                    j = it * 16 + u
                    row = index[base + j]
                    row = jnp.where(flags[row] != 0, row, blank)
                    out[j] = table[row]
                return 0

            lax.fori_loop(0, GATHER // 16, copy_rows, 0)

        first += count


def gather_rows(table, flags, index, phases):
    kinds = table.shape[1]
    steps = sum(phases) // GATHER
    out_specs, first = [], 0
    for count in phases:
        n = count // GATHER
        out_specs.append(
            pl.BlockSpec((GATHER, kinds, LANES), lambda i, lo=first, n=n: (jnp.clip(i - lo, 0, n - 1), 0, 0))
        )
        first += n
    return pl.pallas_call(
        functools.partial(gather_kernel, phases=phases),
        grid=(steps,),
        in_specs=[
            pl.BlockSpec(memory_space=pltpu.SMEM),
            pl.BlockSpec(memory_space=pltpu.SMEM),
            pl.BlockSpec(memory_space=pltpu.VMEM),
        ],
        out_specs=out_specs,
        out_shape=[jax.ShapeDtypeStruct((count, kinds, LANES), table.dtype) for count in phases],
        compiler_params=pltpu.CompilerParams(
            dimension_semantics=("arbitrary",), vmem_limit_bytes=8 * 1024 * 1024
        ),
    )(index, flags, table)


def triangle_kernel(ab, ac, bc, sums, spec, wide, line):
    kinds = ab.shape[1]
    chunks = kinds // 2
    group = 16

    @pl.when(pl.program_id(0) == 0)
    def _():
        spec[...] = jnp.zeros(spec.shape, spec.dtype)

    def fold(x):
        return x[:8] + x[8:]

    def some(it, acc):
        acc = list(acc)
        for u in range(2):
            start = pl.multiple_of((it * 2 + u) * group, group)
            for e, ref in enumerate((ab, bc, ac)):
                rows = ref[pl.ds(start, group)].astype(jnp.float32)
                wide[u, e] = rows.reshape(group * kinds, LANES)
            total_real = total_imag = None
            for c in range(chunks):
                (a_r, a_i), (b_r, b_i), (c_r, c_i) = [
                    [wide[u, e, pl.ds(2 * c + plane, group, stride=kinds), :] for plane in range(2)]
                    for e in range(3)
                ]
                p_r = a_r * b_r - a_i * b_i
                p_i = a_r * b_i + a_i * b_r
                real = p_r * c_r + p_i * c_i
                imag = p_i * c_r - p_r * c_i
                norm = jnp.sqrt(real * real + imag * imag)
                acc[3 * c] = acc[3 * c] + fold(real)
                acc[3 * c + 1] = acc[3 * c + 1] + fold(imag)
                acc[3 * c + 2] = acc[3 * c + 2] + fold(norm)
                total_real = real if c == 0 else total_real + real
                total_imag = imag if c == 0 else total_imag + imag
            line[0, pl.ds(start, group), :] = total_real
            line[1, pl.ds(start, group), :] = total_imag
        return tuple(acc)

    zero = jnp.zeros((8, LANES), jnp.float32)
    acc = lax.fori_loop(0, BLOCK // (2 * group), some, (zero,) * (3 * chunks))
    for c in range(chunks):
        for part in range(3):
            spec[part, c] = spec[part, c] + acc[3 * c + part]
    ones = jnp.ones((8, LANES), jnp.float32)
    for part in range(2):
        lane_sum = lax.dot_general(
            ones,
            line[part],
            (((1,), (1,)), ((), ())),
            precision=lax.Precision.HIGHEST,
            preferred_element_type=jnp.float32,
        )
        sums[pl.ds(part, 1), :] = lane_sum[:1]


def triangle_sums(own, bc, first, second):
    count, kinds, _ = bc.shape
    n = count // BLOCK
    first, second = first // BLOCK, second // BLOCK
    block = (BLOCK, kinds, LANES)
    return pl.pallas_call(
        triangle_kernel,
        grid=(n,),
        in_specs=[
            pl.BlockSpec(block, lambda i: (first + i, 0, 0)),
            pl.BlockSpec(block, lambda i: (second + i, 0, 0)),
            pl.BlockSpec(block, lambda i: (i, 0, 0)),
        ],
        out_specs=[
            pl.BlockSpec((2, BLOCK), lambda i: (0, i)),
            pl.BlockSpec((3, kinds // 2, 8, LANES), lambda i: (0, 0, 0, 0)),
        ],
        out_shape=[
            jax.ShapeDtypeStruct((2, count), jnp.float32),
            jax.ShapeDtypeStruct((3, kinds // 2, 8, LANES), jnp.float32),
        ],
        scratch_shapes=[
            pltpu.VMEM((2, 3, 16 * kinds, LANES), jnp.float32),
            pltpu.VMEM((2, BLOCK, LANES), jnp.float32),
        ],
        compiler_params=pltpu.CompilerParams(dimension_semantics=("arbitrary",)),
        name="triangle_sums",
    )(own, own, bc)


def finish_kernel(*refs, groups, tiles, counts, bands):
    n = len(counts)
    sums, specs = refs[:n], refs[n : 2 * n]
    means, closure, mean_buf, spec_buf, send_g, recv_g, send_t, recv_t = refs[2 * n :]
    grp, tile = lax.axis_index("grp"), lax.axis_index("tile")
    chunks = specs[0].shape[1]
    peers = [(lax.rem(grp + k, groups), tile) for k in range(1, groups)]
    others = [(grp, lax.rem(tile + k, tiles)) for k in range(1, tiles)]
    barrier = pltpu.get_barrier_semaphore()
    for device in peers + others:
        pl.semaphore_signal(barrier, inc=1, device_id=device, device_id_type=pl.DeviceIdType.MESH)
    for part in range(3):
        for c in range(chunks):
            total = specs[0][part, c]
            for spec in specs[1:]:
                total = total + spec[part, c]
            spec_buf[0, pl.ds(part * chunks + c, 1), :] = jnp.sum(total, 0, keepdims=True)
    at = 0
    for ref, count in zip(sums, counts):
        mean_buf[0, :, pl.ds(at, count)] = ref[...]
        at += count
    pl.semaphore_wait(barrier, len(peers) + len(others))
    copies = []
    for buf, send, recv, devices in ((mean_buf, send_g, recv_g, peers), (spec_buf, send_t, recv_t, others)):
        for k, device in enumerate(devices, 1):
            copy = pltpu.make_async_remote_copy(
                src_ref=buf.at[0],
                dst_ref=buf.at[k],
                send_sem=send.at[k],
                recv_sem=recv.at[k],
                device_id=device,
                device_id_type=pl.DeviceIdType.MESH,
            )
            copy.start()
            copies.append(copy)
    for copy in copies:
        copy.wait()
    total = mean_buf[0]
    for k in range(1, groups):
        total = total + mean_buf[k]
    means[...] = total / bands
    total = spec_buf[0]
    for k in range(1, tiles):
        total = total + spec_buf[k]
    norm = 1.0 + total[2 * chunks :]
    closure[pl.ds(0, chunks), :] = total[:chunks] / norm
    closure[pl.ds(chunks, chunks), :] = total[chunks : 2 * chunks] / norm


def finish(sums, specs, groups, tiles, bands):
    counts = tuple(x.shape[1] for x in sums)
    chunks = specs[0].shape[1]
    vmem = pl.BlockSpec(memory_space=pltpu.VMEM)
    return pl.pallas_call(
        functools.partial(finish_kernel, groups=groups, tiles=tiles, counts=counts, bands=bands),
        in_specs=[vmem] * (2 * len(counts)),
        out_specs=[vmem, vmem],
        out_shape=[
            jax.ShapeDtypeStruct((2, sum(counts)), jnp.float32),
            jax.ShapeDtypeStruct((2 * chunks, LANES), jnp.float32),
        ],
        scratch_shapes=[
            pltpu.VMEM((groups, 2, sum(counts)), jnp.float32),
            pltpu.VMEM((tiles, 3 * chunks, LANES), jnp.float32),
            pltpu.SemaphoreType.DMA((groups,)),
            pltpu.SemaphoreType.DMA((groups,)),
            pltpu.SemaphoreType.DMA((tiles,)),
            pltpu.SemaphoreType.DMA((tiles,)),
        ],
        compiler_params=pltpu.CompilerParams(collective_id=0, has_side_effects=True),
        name="finish",
    )(*sums, *specs)


def body(visibility, dish_pair_okay, triangles):
    _, block_rows, cols, channels = visibility.shape
    levels = triangles.shape[1] // TRI_LVL
    tiles, groups = lax.axis_size("tile"), lax.axis_size("grp")
    device = lax.axis_index("tile")
    asked, own = [], []
    for level in range(levels):
        block = triangles[:, level * TRI_LVL : (level + 1) * TRI_LVL]
        partner = jnp.bitwise_xor(device, 1 << level)
        first_local = block[0] - device * block_rows
        second_local = block[1] - partner * block_rows
        asked.append(swapped(second_local * cols + block[2], "tile", level))
        own += [first_local * cols + block[1], first_local * cols + block[2]]
    flags = dish_pair_okay.reshape(-1)
    last = levels - 1
    near_index = jnp.concatenate(asked[:last] + own)
    visibility, far_index, near_index, flags = lax.optimization_barrier((visibility, asked[last], near_index, flags))
    table = turned(visibility)
    pieces = (GATHER,) * (TRI_LVL // GATHER)
    far = gather_rows(table, flags, far_index, pieces)
    far, near_index = lax.optimization_barrier((far, near_index))
    sent = []
    for rows in far:
        sent.append(swapped(rows, "tile", last))
    far = sent
    phases = (TRI_LVL,) * last + (2 * levels * TRI_LVL,)
    *near, own_rows = gather_rows(table, flags, near_index, phases)
    near = [swapped(rows, "tile", level) for level, rows in enumerate(near)]
    parts = []
    for at, rows in [(level * TRI_LVL, rows) for level, rows in enumerate(near)] + [
        (last * TRI_LVL + k * GATHER, rows) for k, rows in enumerate(far)
    ]:
        level, rest = at // TRI_LVL, at % TRI_LVL
        part = triangle_sums(own_rows, rows, 2 * level * TRI_LVL + rest, (2 * level + 1) * TRI_LVL + rest)
        own_rows, part = lax.optimization_barrier((own_rows, part))
        parts.append(part)
    triangle_means, closure = finish(
        [sums for sums, _ in parts], [spec for _, spec in parts], groups, tiles, channels * groups
    )
    width = channels // tiles
    closure_spectrum = lax.dynamic_slice_in_dim(closure.reshape(2, channels), device * width, width, 1)
    return (triangle_means, closure_spectrum)


def solution(mesh):
    placed = (P(None, "tile", None, "grp"), P("tile", None), P(None, "tile"))

    return jax.shard_map(
        body,
        mesh=mesh,
        in_specs=placed,
        out_specs=(P(None, "tile"), P(None, ("grp", "tile"))),
        check_vma=False,
    )
```
